32 devices in a mesh: pairs: 8 (over z, y), gvec: 4 (over x, core).
Axes of the slice: x: 2, y: 2, z: 4, core: 2. Of those that a mesh axis runs over, the one named last changes fastest.
Arguments:
- elements: bfloat16 [16384, 3072], P('pairs', 'gvec'), may hold values from -0.3984375 to 0.3984375
- energy_index: int32 [16384], P('pairs'), may hold values from 0 to 63
Outputs:
- chi_window: float32 [192, 3072], P('pairs', 'gvec')
The draws below stay inside these ranges and needn't reach their ends.
All inputs are finite; a program needn't handle non-finite values.
Results may differ from the reference program's by a relative error of at most 0.0018.
Values may be sent and summed in bfloat16 or wider, within the bound.
A program may use at most 64 MiB of HBM per device.

```python
import jax
import jax.numpy as jnp
from jax import lax

G_DEV = 768
PW_DEV = 48
LEVELS = 64
PAIRS = 16384
NG = 3072
NW = 192
N_GVEC = 4


def set_ends(drawn, stream_key, least, top_value):
    index_at = [jax.random.randint(jax.random.fold_in(stream_key, axis), (), 0, length) for axis, length in enumerate(drawn.shape)]
    main_axis = drawn.shape.index(max(drawn.shape))
    next_to = index_at[:main_axis] + [(index_at[main_axis] + 1) % drawn.shape[main_axis]] + index_at[main_axis + 1:]
    return drawn.at[tuple(index_at)].set(least).at[tuple(next_to)].set(top_value)


def steps_of(rng, dims, pieces, smallest, largest):
    level = 1.0
    for axis_at, blocks in pieces:
        steps = jax.random.uniform(jax.random.fold_in(jax.random.fold_in(rng, 6), axis_at), (blocks,), jnp.float32, smallest / len(pieces), largest / len(pieces))
        level = level * jnp.repeat(jnp.exp(steps), dims[axis_at] // blocks).reshape((-1,) + (1,) * (len(dims) - 1 - axis_at))
    return level


def normal_values(key, extent, deviation, reach, pieces=(), kind=jnp.bfloat16):
    entries = deviation * jax.random.normal(key, extent, jnp.float32)
    if pieces:
        entries = entries * steps_of(key, extent, pieces, -0.22, 0.18)
    return jnp.clip(entries, -reach, reach).astype(kind)


def setup_inputs(seed: int = 0) -> dict:
    arg_keys = jax.random.split(jax.random.key(seed), 3)
    elements = normal_values(arg_keys[0], (PAIRS, NG), 0.05, 0.3984375, ((0, 8), (1, 4)))
    energy_index = set_ends(jax.random.randint(arg_keys[1], (PAIRS,), 0, LEVELS), jax.random.fold_in(arg_keys[1], 1), 0, LEVELS - 1).astype(jnp.int32)
    return {"elements": elements, "energy_index": energy_index}


def make_table():
    steps_k = jnp.arange(LEVELS, dtype=jnp.float32)
    delta = 0.2 * jnp.exp(steps_k * (jnp.log(jnp.float32(50.0)) / (LEVELS - 1)))
    return -2.0 / delta


def reference(elements, energy_index):
    table = make_table()
    weight = table[energy_index]
    scaled = (weight[:, None] * elements.astype(jnp.float32)).astype(jnp.bfloat16)
    panel = elements.reshape(PAIRS, N_GVEC, G_DEV)[:, :, :PW_DEV].reshape(PAIRS, NW)
    return lax.dot_general(panel, scaled, (((0,), (0,)), ((), ())), preferred_element_type=jnp.float32)
```

```python
import functools

import jax
import jax.numpy as jnp
from jax import lax
from jax.experimental import pallas as pl
from jax.experimental.pallas import tpu as pltpu
from jax.sharding import PartitionSpec as P

PW_DEV = 48
LEVELS = 64
MESH = pl.DeviceIdType.MESH


def weights_of(index):
    delta = 0.2 * jnp.exp(
        index.astype(jnp.float32) * (jnp.log(jnp.float32(50.0)) / (LEVELS - 1))
    )
    return -2.0 / delta


def kernel(
    n_pairs, n_gvec, el_hbm, idx_ref, out_ref,
    el, sc, panels, acc, own, sent, got,
    load_sem, gsend_sem, grecv_sem, ssend_sem, srecv_sem,
):
    pw = PW_DEV
    n_p, n_g = el.shape
    half = n_g // 2
    rows = n_gvec * pw // n_pairs
    n_chip = n_gvec // 2
    streamed = pw % rows == 0
    me_p, me_g = lax.axis_index("pairs"), lax.axis_index("gvec")
    chip, core = me_g // 2, lax.rem(me_g, 2)
    partner = chip * 2 + 1 - core

    barrier = pltpu.get_barrier_semaphore()
    for d in range(1, n_pairs):
        pl.semaphore_signal(
            barrier, inc=1, device_id=(lax.rem(me_p + d, n_pairs), me_g), device_id_type=MESH
        )
    for q in range(1, n_chip):
        pl.semaphore_signal(
            barrier, inc=1, device_id=(me_p, lax.rem(chip + q, n_chip) * 2 + core), device_id_type=MESH
        )
    pl.semaphore_signal(barrier, inc=1, device_id=(me_p, partner), device_id_type=MESH)

    stripe = pltpu.make_async_copy(el_hbm.at[:, :128], el.at[:, :128], load_sem.at[0])
    stripe.start()
    n_load = load_sem.shape[0] - 1
    step = n_p // n_load
    loads = []
    for k in range(n_load):
        at = pl.ds(k * step, step)
        loads.append(
            pltpu.make_async_copy(el_hbm.at[at, 128:], el.at[at, 128:], load_sem.at[1 + k])
        )
        loads[-1].start()

    weight = weights_of(idx_ref[...]).T

    def push(source, slot, to_g, n):
        return pltpu.make_async_remote_copy(
            src_ref=panels.at[source], dst_ref=panels.at[source],
            send_sem=gsend_sem.at[n], recv_sem=grecv_sem.at[slot],
            device_id=(me_p, to_g), device_id_type=MESH,
        )

    stripe.wait()
    for k in range(n_p // 128):
        at = pl.ds(k * 128, 128)
        panels[me_g, :, at] = el[at, :128].T[:pw]

    pl.semaphore_wait(barrier, n_pairs - 1 + n_chip)
    first = [push(me_g, me_g, lax.rem(chip + q, n_chip) * 2 + core, q) for q in range(1, n_chip)]
    first.append(push(me_g, me_g, partner, 0))
    for copy in first:
        copy.start()

    per = step // 128
    for k in range(n_p // 128):
        if k % per == 0:
            loads[k // per].wait()
        at = pl.ds(k * 128, 128)
        sc[at, :] = (weight[:, k:k + 1] * el[at, :].astype(jnp.float32)).astype(jnp.bfloat16)

    def send_to(to):
        return pltpu.make_async_remote_copy(
            src_ref=sent.at[to], dst_ref=got.at[me_p],
            send_sem=ssend_sem.at[to], recv_sem=srecv_sem.at[me_p],
            device_id=(to, me_g), device_id_type=MESH,
        )

    def emit(to, block):
        stacked = jnp.concatenate([block[:, :half], block[:, half:]], axis=0)

        @pl.when(to == me_p)
        def _():
            own[...] = stacked

        @pl.when(to != me_p)
        def _():
            sent[to] = stacked.astype(jnp.bfloat16)
            send_to(to).start()

    def tile_of(g):
        tile = jnp.dot(panels[g], sc[...], preferred_element_type=jnp.float32)
        if streamed:
            for b in range(pw // rows):
                emit(g * (pw // rows) + b, tile[b * rows:(b + 1) * rows])
        else:
            acc[pl.ds(pl.multiple_of(g * pw, 8), pw), :] = tile

    def arrived(g):
        push(g, g, partner, 0).wait_recv()

    tile_of(me_g)
    arrived(partner)
    tile_of(partner)

    def other_chip(q):
        g = lax.rem(chip + n_chip - q, n_chip) * 2
        arrived(g + core)
        push(g + core, g + core, partner, n_chip + q).start()
        tile_of(g + core)
        arrived(g + 1 - core)
        tile_of(g + 1 - core)

    if n_chip <= 2:
        for q in range(1, n_chip):
            other_chip(q)
    else:
        pl.loop(1, n_chip)(other_chip)
    if not streamed:
        for k in range(n_pairs):
            emit(k, acc[k * rows:(k + 1) * rows, :])

    total = own[...]
    for d in range(1, n_pairs):
        source = lax.rem(me_p + d, n_pairs)
        pltpu.make_async_remote_copy(
            src_ref=sent.at[source], dst_ref=got.at[source],
            send_sem=ssend_sem.at[source], recv_sem=srecv_sem.at[source],
            device_id=(source, me_g), device_id_type=MESH,
        ).wait_recv()
        total = total + got[source].astype(jnp.float32)
    out_ref[:, :half] = total[:rows]
    out_ref[:, half:] = total[rows:]

    for copy in first:
        copy.wait_send()
    for q in range(1, n_chip):
        push(me_g, me_g, partner, n_chip + q).wait_send()
    for d in range(1, n_pairs):
        send_to(lax.rem(me_p + d, n_pairs)).wait_send()


def shards(n_pairs, n_gvec, elements, energy_index):
    n_p, n_g = elements.shape
    rows = n_gvec * PW_DEV // n_pairs
    streamed = PW_DEV % rows == 0
    half = n_g // 2
    n_load = 8
    vmem = pltpu.VMEM
    dma = pltpu.SemaphoreType.DMA
    return pl.pallas_call(
        functools.partial(kernel, n_pairs, n_gvec),
        out_shape=jax.ShapeDtypeStruct((rows, n_g), jnp.float32),
        in_specs=[
            pl.BlockSpec(memory_space=pl.ANY),
            pl.BlockSpec(memory_space=vmem),
        ],
        out_specs=pl.BlockSpec(memory_space=vmem),
        scratch_shapes=[
            vmem((n_p, n_g), jnp.bfloat16),
            vmem((n_p, n_g), jnp.bfloat16),
            vmem((n_gvec, PW_DEV, n_p), jnp.bfloat16),
            vmem((8 if streamed else n_gvec * PW_DEV, n_g), jnp.float32),
            vmem((2 * rows, half), jnp.float32),
            vmem((n_pairs, 2 * rows, half), jnp.bfloat16),
            vmem((n_pairs, 2 * rows, half), jnp.bfloat16),
            dma((1 + n_load,)),
            dma((n_gvec,)),
            dma((n_gvec,)),
            dma((n_pairs,)),
            dma((n_pairs,)),
        ],
        compiler_params=pltpu.CompilerParams(collective_id=0, has_side_effects=True),
    )(elements, energy_index.reshape(n_p // 128, 128))


def solution(mesh):
    placed = (P("pairs", "gvec"), P("pairs"))
    body = functools.partial(shards, mesh.shape["pairs"], mesh.shape["gvec"])
    return jax.shard_map(
        body, mesh=mesh, in_specs=placed, out_specs=P("pairs", "gvec"), check_vma=False
    )
```

```python
import functools

import jax
import jax.numpy as jnp
from jax import lax
from jax.experimental import pallas as pl
from jax.experimental.pallas import tpu as pltpu
from jax.sharding import PartitionSpec as P

PW_DEV = 48
LEVELS = 64
MESH = pl.DeviceIdType.MESH


def weights_of(index):
    delta = 0.2 * jnp.exp(
        index.astype(jnp.float32) * (jnp.log(jnp.float32(50.0)) / (LEVELS - 1))
    )
    return -2.0 / delta


def kernel(
    n_pairs, n_gvec, el_hbm, idx_ref, out_ref,
    el, sc, panels, acc, own, sent, got,
    load_sem, gsend_sem, grecv_sem, ssend_sem, srecv_sem,
):
    pw = PW_DEV
    n_p, n_g = el.shape
    half = n_g // 2
    rows = n_gvec * pw // n_pairs
    n_chip = n_gvec // 2
    streamed = pw % rows == 0
    me_p, me_g = lax.axis_index("pairs"), lax.axis_index("gvec")
    chip, core = me_g // 2, lax.rem(me_g, 2)
    partner = chip * 2 + 1 - core

    barrier = pltpu.get_barrier_semaphore()
    for d in range(1, n_pairs):
        pl.semaphore_signal(
            barrier, inc=1, device_id=(lax.rem(me_p + d, n_pairs), me_g), device_id_type=MESH
        )
    for q in range(1, n_chip):
        pl.semaphore_signal(
            barrier, inc=1, device_id=(me_p, lax.rem(chip + q, n_chip) * 2 + core), device_id_type=MESH
        )
    pl.semaphore_signal(barrier, inc=1, device_id=(me_p, partner), device_id_type=MESH)

    stripe = pltpu.make_async_copy(el_hbm.at[:, :128], el.at[:, :128], load_sem.at[0])
    stripe.start()
    n_load = load_sem.shape[0] - 1
    step = n_p // n_load
    loads = []
    for k in range(n_load):
        at = pl.ds(k * step, step)
        loads.append(
            pltpu.make_async_copy(el_hbm.at[at, 128:], el.at[at, 128:], load_sem.at[1 + k])
        )
        loads[-1].start()

    weight = weights_of(idx_ref[...]).T

    def push(source, slot, to_g, n):
        return pltpu.make_async_remote_copy(
            src_ref=panels.at[source], dst_ref=panels.at[source],
            send_sem=gsend_sem.at[n], recv_sem=grecv_sem.at[slot],
            device_id=(me_p, to_g), device_id_type=MESH,
        )

    stripe.wait()
    for k in range(n_p // 128):
        at = pl.ds(k * 128, 128)
        panels[me_g, :, at] = el[at, :128].T[:pw]

    pl.semaphore_wait(barrier, n_pairs - 1 + n_chip)
    first = [push(me_g, me_g, lax.rem(chip + q, n_chip) * 2 + core, q) for q in range(1, n_chip)]
    first.append(push(me_g, me_g, partner, 0))
    for copy in first:
        copy.start()

    per = step // 128
    for k in range(n_p // 128):
        if k % per == 0:
            loads[k // per].wait()
        at = pl.ds(k * 128, 128)
        sc[at, :] = (weight[:, k:k + 1] * el[at, :].astype(jnp.float32)).astype(jnp.bfloat16)

    def send_to(to):
        return pltpu.make_async_remote_copy(
            src_ref=sent.at[to], dst_ref=got.at[me_p],
            send_sem=ssend_sem.at[to], recv_sem=srecv_sem.at[me_p],
            device_id=(to, me_g), device_id_type=MESH,
        )

    def emit(to, block):
        stacked = jnp.concatenate([block[:, :half], block[:, half:]], axis=0)

        @pl.when(to == me_p)
        def _():
            own[...] = stacked

        @pl.when(to != me_p)
        def _():
            sent[to] = stacked.astype(jnp.bfloat16)
            send_to(to).start()

    def tile_of(g):
        tile = jnp.dot(panels[g], sc[...], preferred_element_type=jnp.float32)
        if streamed:
            for b in range(pw // rows):
                emit(g * (pw // rows) + b, tile[b * rows:(b + 1) * rows])
        else:
            acc[pl.ds(pl.multiple_of(g * pw, 8), pw), :] = tile

    def arrived(g):
        push(g, g, partner, 0).wait_recv()

    tile_of(me_g)
    arrived(partner)
    tile_of(partner)

    def other_chip(q):
        g = lax.rem(chip + n_chip - q, n_chip) * 2
        arrived(g + core)
        push(g + core, g + core, partner, n_chip + q).start()
        tile_of(g + core)
        arrived(g + 1 - core)
        tile_of(g + 1 - core)

    if n_chip <= 2:
        for q in range(1, n_chip):
            other_chip(q)
    else:
        pl.loop(1, n_chip)(other_chip)
    if not streamed:
        for k in range(n_pairs):
            emit(k, acc[k * rows:(k + 1) * rows, :])

    total = own[...]
    for d in range(1, n_pairs):
        source = lax.rem(me_p + d, n_pairs)
        pltpu.make_async_remote_copy(
            src_ref=sent.at[source], dst_ref=got.at[source],
            send_sem=ssend_sem.at[source], recv_sem=srecv_sem.at[source],
            device_id=(source, me_g), device_id_type=MESH,
        ).wait_recv()
        total = total + got[source].astype(jnp.float32)
    out_ref[:, :half] = total[:rows]
    out_ref[:, half:] = total[rows:]

    for copy in first:
        copy.wait_send()
    for q in range(1, n_chip):
        push(me_g, me_g, partner, n_chip + q).wait_send()
    for d in range(1, n_pairs):
        send_to(lax.rem(me_p + d, n_pairs)).wait_send()


def shards(n_pairs, n_gvec, elements, energy_index):
    n_p, n_g = elements.shape
    rows = n_gvec * PW_DEV // n_pairs
    streamed = PW_DEV % rows == 0
    half = n_g // 2
    n_load = 8
    vmem = pltpu.VMEM
    dma = pltpu.SemaphoreType.DMA
    return pl.pallas_call(
        functools.partial(kernel, n_pairs, n_gvec),
        out_shape=pltpu.VMEM((rows, n_g), jnp.float32),
        in_specs=[
            pl.BlockSpec(memory_space=pl.ANY),
            pl.BlockSpec(memory_space=vmem),
        ],
        out_specs=pl.BlockSpec(memory_space=vmem),
        scratch_shapes=[
            vmem((n_p, n_g), jnp.bfloat16),
            vmem((n_p, n_g), jnp.bfloat16),
            vmem((n_gvec, PW_DEV, n_p), jnp.bfloat16),
            vmem((8 if streamed else n_gvec * PW_DEV, n_g), jnp.float32),
            vmem((2 * rows, half), jnp.float32),
            vmem((n_pairs, 2 * rows, half), jnp.bfloat16),
            vmem((n_pairs, 2 * rows, half), jnp.bfloat16),
            dma((1 + n_load,)),
            dma((n_gvec,)),
            dma((n_gvec,)),
            dma((n_pairs,)),
            dma((n_pairs,)),
        ],
        compiler_params=pltpu.CompilerParams(collective_id=0, has_side_effects=True),
    )(elements, energy_index.reshape(n_p // 128, 128))


def solution(mesh):
    placed = (P("pairs", "gvec"), P("pairs"))
    body = functools.partial(shards, mesh.shape["pairs"], mesh.shape["gvec"])
    return jax.shard_map(
        body, mesh=mesh, in_specs=placed, out_specs=P("pairs", "gvec"), check_vma=False
    )
```

```python
import functools

import jax
import jax.numpy as jnp
from jax import lax
from jax.experimental import pallas as pl
from jax.experimental.pallas import tpu as pltpu
from jax.sharding import PartitionSpec as P

PW_DEV = 48
LEVELS = 64
MESH = pl.DeviceIdType.MESH


def weights_of(index):
    delta = 0.2 * jnp.exp(
        index.astype(jnp.float32) * (jnp.log(jnp.float32(50.0)) / (LEVELS - 1))
    )
    return -2.0 / delta


def kernel(
    n_pairs, n_gvec, el_hbm, idx_hbm, out_ref,
    idx, el, sc, panels, acc, own, sent, got,
    load_sem, gsend_sem, grecv_sem, ssend_sem, srecv_sem,
):
    pw = PW_DEV
    n_p, n_g = el.shape
    half = n_g // 2
    rows = n_gvec * pw // n_pairs
    n_chip = n_gvec // 2
    streamed = pw % rows == 0
    index = pltpu.make_async_copy(idx_hbm, idx, load_sem.at[0])
    me_p, me_g = lax.axis_index("pairs"), lax.axis_index("gvec")
    chip, core = me_g // 2, lax.rem(me_g, 2)
    partner = chip * 2 + 1 - core

    stripe = pltpu.make_async_copy(el_hbm.at[:, :128], el.at[:, :128], load_sem.at[1])
    stripe.start()
    index.start()
    n_load = load_sem.shape[0] - 2
    step = n_p // n_load
    loads = []
    for k in range(n_load):
        at = pl.ds(k * step, step)
        loads.append(
            pltpu.make_async_copy(el_hbm.at[at, 128:], el.at[at, 128:], load_sem.at[2 + k])
        )
        loads[-1].start()

    barrier = pltpu.get_barrier_semaphore()
    for d in range(1, n_pairs):
        pl.semaphore_signal(
            barrier, inc=1, device_id=(lax.rem(me_p + d, n_pairs), me_g), device_id_type=MESH
        )
    for q in range(1, n_chip):
        pl.semaphore_signal(
            barrier, inc=1, device_id=(me_p, lax.rem(chip + q, n_chip) * 2 + core), device_id_type=MESH
        )
    pl.semaphore_signal(barrier, inc=1, device_id=(me_p, partner), device_id_type=MESH)

    def push(source, slot, to_g, n):
        return pltpu.make_async_remote_copy(
            src_ref=panels.at[source], dst_ref=panels.at[source],
            send_sem=gsend_sem.at[n], recv_sem=grecv_sem.at[slot],
            device_id=(me_p, to_g), device_id_type=MESH,
        )

    stripe.wait()
    for k in range(n_p // 128):
        at = pl.ds(k * 128, 128)
        panels[me_g, :, at] = el[at, :128].T[:pw]

    pl.semaphore_wait(barrier, n_pairs - 1 + n_chip)
    first = [push(me_g, me_g, lax.rem(chip + q, n_chip) * 2 + core, q) for q in range(1, n_chip)]
    first.append(push(me_g, me_g, partner, 0))
    for copy in first:
        copy.start()

    index.wait()
    weight = weights_of(idx[...]).T
    per = step // 128
    for k in range(n_p // 128):
        if k % per == 0:
            loads[k // per].wait()
        at = pl.ds(k * 128, 128)
        sc[at, :] = (weight[:, k:k + 1] * el[at, :].astype(jnp.float32)).astype(jnp.bfloat16)

    def send_to(to):
        return pltpu.make_async_remote_copy(
            src_ref=sent.at[to], dst_ref=got.at[me_p],
            send_sem=ssend_sem.at[to], recv_sem=srecv_sem.at[me_p],
            device_id=(to, me_g), device_id_type=MESH,
        )

    def emit(to, block):
        stacked = jnp.concatenate([block[:, :half], block[:, half:]], axis=0)

        @pl.when(to == me_p)
        def _():
            own[...] = stacked

        @pl.when(to != me_p)
        def _():
            sent[to] = stacked.astype(jnp.bfloat16)
            send_to(to).start()

    def tile_of(g):
        tile = jnp.dot(panels[g], sc[...], preferred_element_type=jnp.float32)
        if streamed:
            for b in range(pw // rows):
                emit(g * (pw // rows) + b, tile[b * rows:(b + 1) * rows])
        else:
            acc[pl.ds(pl.multiple_of(g * pw, 8), pw), :] = tile

    def arrived(g):
        push(g, g, partner, 0).wait_recv()

    tile_of(me_g)
    arrived(partner)
    tile_of(partner)

    def other_chip(q):
        g = lax.rem(chip + n_chip - q, n_chip) * 2
        arrived(g + core)
        push(g + core, g + core, partner, n_chip + q).start()
        tile_of(g + core)
        arrived(g + 1 - core)
        tile_of(g + 1 - core)

    if n_chip <= 2:
        for q in range(1, n_chip):
            other_chip(q)
    else:
        pl.loop(1, n_chip)(other_chip)
    if not streamed:
        for k in range(n_pairs):
            emit(k, acc[k * rows:(k + 1) * rows, :])

    total = own[...]
    for d in range(1, n_pairs):
        source = lax.rem(me_p + d, n_pairs)
        pltpu.make_async_remote_copy(
            src_ref=sent.at[source], dst_ref=got.at[source],
            send_sem=ssend_sem.at[source], recv_sem=srecv_sem.at[source],
            device_id=(source, me_g), device_id_type=MESH,
        ).wait_recv()
        total = total + got[source].astype(jnp.float32)
    out_ref[:, :half] = total[:rows]
    out_ref[:, half:] = total[rows:]

    for copy in first:
        copy.wait_send()
    for q in range(1, n_chip):
        push(me_g, me_g, partner, n_chip + q).wait_send()
    for d in range(1, n_pairs):
        send_to(lax.rem(me_p + d, n_pairs)).wait_send()


def shards(n_pairs, n_gvec, elements, energy_index):
    n_p, n_g = elements.shape
    rows = n_gvec * PW_DEV // n_pairs
    streamed = PW_DEV % rows == 0
    half = n_g // 2
    n_load = 8
    vmem = pltpu.VMEM
    dma = pltpu.SemaphoreType.DMA
    return pl.pallas_call(
        functools.partial(kernel, n_pairs, n_gvec),
        out_shape=pltpu.VMEM((rows, n_g), jnp.float32),
        in_specs=[
            pl.BlockSpec(memory_space=pl.ANY),
            pl.BlockSpec(memory_space=pl.ANY),
        ],
        out_specs=pl.BlockSpec(memory_space=vmem),
        scratch_shapes=[
            vmem((n_p // 128, 128), jnp.int32),
            vmem((n_p, n_g), jnp.bfloat16),
            vmem((n_p, n_g), jnp.bfloat16),
            vmem((n_gvec, PW_DEV, n_p), jnp.bfloat16),
            vmem((8 if streamed else n_gvec * PW_DEV, n_g), jnp.float32),
            vmem((2 * rows, half), jnp.float32),
            vmem((n_pairs, 2 * rows, half), jnp.bfloat16),
            vmem((n_pairs, 2 * rows, half), jnp.bfloat16),
            dma((2 + n_load,)),
            dma((n_gvec,)),
            dma((n_gvec,)),
            dma((n_pairs,)),
            dma((n_pairs,)),
        ],
        compiler_params=pltpu.CompilerParams(collective_id=0, has_side_effects=True),
    )(elements, energy_index.reshape(n_p // 128, 128))


def solution(mesh):
    placed = (P("pairs", "gvec"), P("pairs"))
    body = functools.partial(shards, mesh.shape["pairs"], mesh.shape["gvec"])
    return jax.shard_map(
        body, mesh=mesh, in_specs=placed, out_specs=P("pairs", "gvec"), check_vma=False
    )
```

```python
import functools

import jax
import jax.numpy as jnp
from jax import lax
from jax.experimental import pallas as pl
from jax.experimental.pallas import tpu as pltpu
from jax.sharding import PartitionSpec as P

PW_DEV = 48
LEVELS = 64
MESH = pl.DeviceIdType.MESH


def weights_of(index):
    delta = 0.2 * jnp.exp(
        index.astype(jnp.float32) * (jnp.log(jnp.float32(50.0)) / (LEVELS - 1))
    )
    return -2.0 / delta


def kernel(
    n_pairs, n_gvec, el_hbm, idx_hbm, out_ref,
    idx, el, sc, panels, acc, own, sent, got,
    load_sem, gsend_sem, grecv_sem, ssend_sem, srecv_sem,
):
    pw = PW_DEV
    n_p, n_g = el.shape
    half = n_g // 2
    rows = n_gvec * pw // n_pairs
    n_chip = n_gvec // 2
    streamed = pw % rows == 0
    index = pltpu.make_async_copy(idx_hbm, idx, load_sem.at[0])
    me_p, me_g = lax.axis_index("pairs"), lax.axis_index("gvec")
    chip, core = me_g // 2, lax.rem(me_g, 2)
    partner = chip * 2 + 1 - core

    stripe = pltpu.make_async_copy(el_hbm.at[:, :128], el.at[:, :128], load_sem.at[1])
    stripe.start()
    index.start()
    n_load = load_sem.shape[0] - 2
    step = n_p // n_load
    loads = []
    for k in range(n_load):
        at = pl.ds(k * step, step)
        loads.append(
            pltpu.make_async_copy(el_hbm.at[at, 128:], el.at[at, 128:], load_sem.at[2 + k])
        )

    barrier = pltpu.get_barrier_semaphore()
    for d in range(1, n_pairs):
        pl.semaphore_signal(
            barrier, inc=1, device_id=(lax.rem(me_p + d, n_pairs), me_g), device_id_type=MESH
        )
    for q in range(1, n_chip):
        pl.semaphore_signal(
            barrier, inc=1, device_id=(me_p, lax.rem(chip + q, n_chip) * 2 + core), device_id_type=MESH
        )
    pl.semaphore_signal(barrier, inc=1, device_id=(me_p, partner), device_id_type=MESH)

    def push(source, slot, to_g, n):
        return pltpu.make_async_remote_copy(
            src_ref=panels.at[source], dst_ref=panels.at[source],
            send_sem=gsend_sem.at[n], recv_sem=grecv_sem.at[slot],
            device_id=(me_p, to_g), device_id_type=MESH,
        )

    stripe.wait()
    for copy in loads:
        copy.start()
    for k in range(n_p // 128):
        at = pl.ds(k * 128, 128)
        panels[me_g, :, at] = el[at, :128].T[:pw]

    pl.semaphore_wait(barrier, n_pairs - 1 + n_chip)
    first = [push(me_g, me_g, lax.rem(chip + q, n_chip) * 2 + core, q) for q in range(1, n_chip)]
    first.append(push(me_g, me_g, partner, 0))
    for copy in first:
        copy.start()

    index.wait()
    weight = weights_of(idx[...]).T
    per = step // 128
    for k in range(n_p // 128):
        if k % per == 0:
            loads[k // per].wait()
        at = pl.ds(k * 128, 128)
        sc[at, :] = (weight[:, k:k + 1] * el[at, :].astype(jnp.float32)).astype(jnp.bfloat16)

    def send_to(to):
        return pltpu.make_async_remote_copy(
            src_ref=sent.at[to], dst_ref=got.at[me_p],
            send_sem=ssend_sem.at[to], recv_sem=srecv_sem.at[me_p],
            device_id=(to, me_g), device_id_type=MESH,
        )

    def emit(to, block):
        stacked = jnp.concatenate([block[:, :half], block[:, half:]], axis=0)

        @pl.when(to == me_p)
        def _():
            own[...] = stacked

        @pl.when(to != me_p)
        def _():
            sent[to] = stacked.astype(jnp.bfloat16)
            send_to(to).start()

    def tile_of(g):
        keep(g, jnp.dot(panels[g], sc[...], preferred_element_type=jnp.float32))

    def keep(g, tile):
        if streamed:
            for b in range(pw // rows):
                emit(g * (pw // rows) + b, tile[b * rows:(b + 1) * rows])
        else:
            acc[pl.ds(pl.multiple_of(g * pw, 8), pw), :] = tile

    def pair_of(c):
        tile = jnp.dot(
            panels[pl.ds(c * 2, 2)].reshape(2 * pw, n_p), sc[...], preferred_element_type=jnp.float32
        )
        for n in range(2):
            keep(c * 2 + n, tile[n * pw:(n + 1) * pw])

    def arrived(g):
        push(g, g, partner, 0).wait_recv()

    arrived(partner)
    pair_of(chip)

    def other_chip(q):
        g = lax.rem(chip + n_chip - q, n_chip) * 2
        arrived(g + core)
        push(g + core, g + core, partner, n_chip + q).start()
        tile_of(g + core)
        arrived(g + 1 - core)
        tile_of(g + 1 - core)

    if n_chip <= 2:
        for q in range(1, n_chip):
            other_chip(q)
    else:
        pl.loop(1, n_chip)(other_chip)
    if not streamed:
        for k in range(n_pairs):
            emit(k, acc[k * rows:(k + 1) * rows, :])

    total = own[...]
    for d in range(1, n_pairs):
        source = lax.rem(me_p + d, n_pairs)
        pltpu.make_async_remote_copy(
            src_ref=sent.at[source], dst_ref=got.at[source],
            send_sem=ssend_sem.at[source], recv_sem=srecv_sem.at[source],
            device_id=(source, me_g), device_id_type=MESH,
        ).wait_recv()
        total = total + got[source].astype(jnp.float32)
    out_ref[:, :half] = total[:rows]
    out_ref[:, half:] = total[rows:]

    for copy in first:
        copy.wait_send()
    for q in range(1, n_chip):
        push(me_g, me_g, partner, n_chip + q).wait_send()
    for d in range(1, n_pairs):
        send_to(lax.rem(me_p + d, n_pairs)).wait_send()


def shards(n_pairs, n_gvec, elements, energy_index):
    n_p, n_g = elements.shape
    rows = n_gvec * PW_DEV // n_pairs
    streamed = PW_DEV % rows == 0
    half = n_g // 2
    n_load = 8
    vmem = pltpu.VMEM
    dma = pltpu.SemaphoreType.DMA
    return pl.pallas_call(
        functools.partial(kernel, n_pairs, n_gvec),
        out_shape=pltpu.VMEM((rows, n_g), jnp.float32),
        in_specs=[
            pl.BlockSpec(memory_space=pl.ANY),
            pl.BlockSpec(memory_space=pl.ANY),
        ],
        out_specs=pl.BlockSpec(memory_space=vmem),
        scratch_shapes=[
            vmem((n_p // 128, 128), jnp.int32),
            vmem((n_p, n_g), jnp.bfloat16),
            vmem((n_p, n_g), jnp.bfloat16),
            vmem((n_gvec, PW_DEV, n_p), jnp.bfloat16),
            vmem((8 if streamed else n_gvec * PW_DEV, n_g), jnp.float32),
            vmem((2 * rows, half), jnp.float32),
            vmem((n_pairs, 2 * rows, half), jnp.bfloat16),
            vmem((n_pairs, 2 * rows, half), jnp.bfloat16),
            dma((2 + n_load,)),
            dma((n_gvec,)),
            dma((n_gvec,)),
            dma((n_pairs,)),
            dma((n_pairs,)),
        ],
        compiler_params=pltpu.CompilerParams(collective_id=0, has_side_effects=True),
    )(elements, energy_index.reshape(n_p // 128, 128))


def solution(mesh):
    placed = (P("pairs", "gvec"), P("pairs"))
    body = functools.partial(shards, mesh.shape["pairs"], mesh.shape["gvec"])
    return jax.shard_map(
        body, mesh=mesh, in_specs=placed, out_specs=P("pairs", "gvec"), check_vma=False
    )
```
